256 devices in a mesh: dp: 2 (over core), expert: 128 (over z, x, y).
Axes of the slice: x: 4, y: 4, z: 8, core: 2. Of those that a mesh axis runs over, the one named last changes fastest.
Arguments:
- tokens: bfloat16 [65536, 1024], P(('dp', 'expert')), may hold values from -6 to 6
- ln_gain: float32 [1024], replicated, may hold values from 0.5 to 1.5
- router_weight: bfloat16 [1024, 128], replicated
- routes_expert: int32 [65536], P(('dp', 'expert')), may hold values from 0 to 127, as said below
- route_slot: int32 [65536], P(('dp', 'expert')), may hold values from -1 to 3, as said below
- w_in: bfloat16 [128, 1024, 4096], P('expert', None, 'dp'), may hold values from -0.1875 to 0.1875
- w_out: bfloat16 [128, 4096, 1024], P('expert', 'dp'), may hold values from -0.09375 to 0.09375
Outputs:
- mixed: bfloat16 [65536, 1024], P(('dp', 'expert'))
- expert_update: bfloat16 [65536, 1024], P(('dp', 'expert'))
The draws below stay inside these ranges and needn't reach their ends.
Inputs may be any that keep to these rules, and one draw needn't show every extreme that they name: `routes_expert`: every expert is chosen by some token. route_slot[t] is the number of earlier tokens of the same device (the same aligned block of 256 tokens) routed to the same expert, or -1 where that number is 4 or more; the value 4 - 1 occurs in every draw.
All inputs are finite; a program needn't handle non-finite values.
Results may differ from the reference program's by a relative error of at most 0.0058.
Values may be sent and summed in bfloat16 or wider, within the bound.
A program may use at most 64 MiB of HBM per device.

```python
import jax
import jax.numpy as jnp
from jax import lax

D = 1024
HID = 4096
CAP = 4
TOK_DEV = 256
EXPERTS = 128
TOKENS = 65536


def route_pair(key):
    key = jax.random.fold_in(key, 11)
    first, second = jax.random.split(key)
    hot_list = jax.random.permutation(first, EXPERTS)[:8].astype(jnp.int32)
    drawn = jax.random.randint(second, (TOKENS,), 0, 4 * EXPERTS).astype(jnp.int32)
    result = drawn % EXPERTS
    hot_pick = hot_list[(drawn - 3 * EXPERTS) % 8]
    chosen = jnp.where(drawn < 3 * EXPERTS, result, hot_pick).astype(jnp.int32)
    blocks = chosen.reshape(TOKENS // TOK_DEV, TOK_DEV)
    onehot = (blocks[:, :, None] == jnp.arange(EXPERTS, dtype=jnp.int32)[None, None, :]).astype(jnp.int32)
    rank = jnp.sum(jnp.cumsum(onehot, axis=1) * onehot, axis=2) - 1
    slots = jnp.where(rank < CAP, rank, -1).astype(jnp.int32).reshape(TOKENS)
    return (chosen, slots)


def draw_routes_expert(key, part):
    return route_pair(key)[0]


def draw_route_slot(key, part):
    return route_pair(key)[1]


def draw_router_weight(key, part):
    key = jax.random.fold_in(key, 23)
    first, second = jax.random.split(key, 2)
    column_scale = jnp.exp(jax.random.uniform(first, (EXPERTS,), jnp.float32, jnp.log(1.0), jnp.log(12.0)))
    entries = jax.random.normal(second, (D, EXPERTS), jnp.float32)
    return (entries * column_scale[None, :] / jnp.sqrt(1.0 * D)).astype(jnp.bfloat16)


def block_scale(rng, extent, cuts, low, top_value):
    def one(dim, shards_of):
        heights = jax.random.uniform(jax.random.fold_in(jax.random.fold_in(rng, 6), dim), (shards_of,), jnp.float32, low / len(cuts), top_value / len(cuts))
        return jnp.repeat(jnp.exp(heights), extent[dim] // shards_of).reshape((-1,) + (1,) * (len(extent) - dim - 1))

    level = one(*cuts[0])
    for cut in cuts[1:]:
        level = level * one(*cut)
    return level


def scatter_about(stream_key, extent, deviation, most, shards=(), kind=jnp.bfloat16):
    level = block_scale(stream_key, extent, shards, -0.22, 0.18) if shards else 1.0
    array = jax.random.normal(stream_key, extent, jnp.float32) * deviation * level
    return jnp.minimum(jnp.maximum(array, -most), most).astype(kind)


def setup_inputs(seed: int = 0) -> dict:
    seeds = jax.random.split(jax.random.key(seed), 8)
    return {
        "tokens": scatter_about(seeds[0], (TOKENS, D), 1.0, 6.0, ((0, 256),)),
        "ln_gain": jnp.clip(1.0 + 0.1 * jax.random.normal(seeds[1], (D,), jnp.float32), 0.5, 1.5),
        "router_weight": draw_router_weight(jax.random.fold_in(seeds[7], 71), 0),
        "routes_expert": draw_routes_expert(jax.random.fold_in(seeds[7], 71), 0),
        "route_slot": draw_route_slot(jax.random.fold_in(seeds[7], 71), 0),
        "w_in": scatter_about(seeds[5], (EXPERTS, D, HID), D ** -0.5, 0.1875, ((0, 128), (2, 2))),
        "w_out": scatter_about(seeds[6], (EXPERTS, HID, D), HID ** -0.5, 0.09375, ((0, 128), (1, 2))),
    }


def reference(tokens, ln_gain, router_weight, routes_expert, route_slot, w_in, w_out):
    values = tokens.astype(jnp.float32)
    mean = lax.optimization_barrier(jnp.mean(values, axis=1, keepdims=True))
    var = lax.optimization_barrier(jnp.mean((values - mean) ** 2, axis=1, keepdims=True))
    normed = ((values - mean) * lax.rsqrt(var + 1e-06) * ln_gain[None, :]).astype(jnp.bfloat16)
    logits = jnp.dot(normed, router_weight, preferred_element_type=jnp.float32)
    probs = jax.nn.softmax(logits, axis=1)
    gate = jnp.take_along_axis(probs, routes_expert[:, None].astype(jnp.int32), axis=1)[:, 0]
    sources = TOKENS // TOK_DEV
    source = (jnp.arange(TOKENS, dtype=jnp.int32) // TOK_DEV).astype(jnp.int32)
    kept = route_slot >= 0
    total_rows = EXPERTS * sources * CAP
    flat = jnp.where(kept, (routes_expert * sources + source) * CAP + route_slot, total_rows).astype(jnp.int32)
    width = tokens.shape[1]
    buffer = jnp.zeros((total_rows, width), jnp.bfloat16).at[flat].set(normed, mode='drop')
    buffer = buffer.reshape(EXPERTS, sources * CAP, width)

    def serve_expert(operands):
        rows, weight_in, weight_out = operands
        hidden = jax.nn.gelu(jnp.dot(rows, weight_in, preferred_element_type=jnp.float32), approximate=True).astype(jnp.bfloat16)
        return jnp.dot(hidden, weight_out, preferred_element_type=jnp.float32).astype(jnp.bfloat16)
    outputs = lax.map(serve_expert, (buffer, w_in, w_out)).reshape(total_rows, width)
    back = outputs[jnp.minimum(flat, total_rows - 1)]
    update = jnp.where(kept[:, None], back, jnp.zeros_like(back))
    mixed = (values + gate[:, None] * update.astype(jnp.float32)).astype(jnp.bfloat16)
    return (mixed, update)
```

```python
import functools

import jax
import jax.numpy as jnp
from jax import lax
from jax.experimental import pallas as pl
from jax.experimental.pallas import tpu as pltpu
from jax.sharding import PartitionSpec as P

CAP = 4
ZS, XS, YS = 8, 4, 4
PLANE = XS * YS
EXPERTS = ZS * PLANE
SLOTS = EXPERTS * CAP
CHUNKS = ((3, 5), (2, 6), (4, 0), (1, 7))
ORDER = tuple(dz for pair in CHUNKS for dz in pair)
SELF = ORDER.index(0) * PLANE
CHUNK_BLOCKS = 2 * PLANE
CHUNK_ROWS = CHUNK_BLOCKS * CAP
TILE = 512
MESH = pl.DeviceIdType.MESH


def kernel(
    tokens, gain, router, experts, slots, w_in, w_out,
    mixed, update,
    send, recv, resp, back, win, wout, normed, acc, gate, onehot,
    load_sem, pair_send, pair_recv, out_send, out_recv, back_send, back_recv,
):
    core = lax.axis_index("dp")
    me = lax.axis_index("expert")
    z, x, y = me // PLANE, lax.rem(me // YS, XS), lax.rem(me, YS)
    half = w_in.shape[2] // TILE

    def at(expert):
        return {"dp": core, "expert": expert}

    def away(dz, j, sign):
        dx, dy = j // YS, lax.rem(j, YS)
        return (
            lax.rem(z + sign * dz + ZS, ZS) * PLANE
            + lax.rem(x + sign * dx + XS, XS) * YS
            + lax.rem(y + sign * dy + YS, YS)
        )

    def blocks(chunk, act):
        for i, dz in enumerate(CHUNKS[chunk]):
            base = (2 * chunk + i) * PLANE

            def step(j, carry):
                act(base + j, dz, j)
                return carry

            lax.fori_loop(1 if dz == 0 else 0, PLANE, step, 0)

    def greet(k, dz, j):
        pl.semaphore_signal(barrier, inc=1, device_id=at(away(dz, j, 1)), device_id_type=MESH)

    loads = []
    for t in range(half):
        cols = pl.ds(t * TILE, TILE)
        loads.append(pltpu.make_async_copy(w_in.at[0, :, cols], win.at[t], load_sem.at[0, t]))
        loads.append(pltpu.make_async_copy(w_out.at[0, cols, :], wout.at[t], load_sem.at[1, t]))
    for copy in loads:
        copy.start()

    barrier = pltpu.get_barrier_semaphore()
    partner = {"dp": 1 - core, "expert": me}
    pl.semaphore_signal(barrier, inc=1, device_id=partner, device_id_type=MESH)
    for chunk in range(len(CHUNKS)):
        blocks(chunk, greet)

    values = tokens[...].astype(jnp.float32)
    mean = jnp.mean(values, axis=1, keepdims=True)
    centred = values - mean
    var = jnp.mean(centred * centred, axis=1, keepdims=True)
    normed[...] = (centred * lax.rsqrt(var + 1e-06) * gain[...]).astype(jnp.bfloat16)

    expert = experts[...]
    slot = slots[...]
    dz = (expert // PLANE - z) & (ZS - 1)
    dx = ((expert // YS) % XS - x) & (XS - 1)
    dy = (expert % YS - y) & (YS - 1)
    place = jnp.zeros_like(dz)
    for i, d in enumerate(ORDER):
        place = jnp.where(dz == d, i, place)
    rel = ((place * PLANE) + dx * YS + dy) * CAP + slot
    rel = jnp.where(slot >= 0, rel, -1)
    count = rel.shape[1]
    for chunk in range(len(CHUNKS)):
        rows = lax.broadcasted_iota(jnp.int32, (CHUNK_ROWS, count), 0) + chunk * CHUNK_ROWS
        pick = jnp.where(rows == rel, 1.0, 0.0).astype(jnp.bfloat16)
        picked = jnp.dot(pick, normed[...], preferred_element_type=jnp.float32)
        first = chunk * CHUNK_BLOCKS
        send[first : first + CHUNK_BLOCKS] = picked.reshape(CHUNK_BLOCKS, CAP, -1).astype(jnp.bfloat16)

    pl.semaphore_wait(barrier, EXPERTS)

    def pair_copy(w, t, which):
        dst = (win, wout)[which].at[half + t]
        src = w.at[0, :, pl.ds(t * TILE, TILE)] if which == 0 else w.at[0, pl.ds(t * TILE, TILE), :]
        return pltpu.make_async_remote_copy(
            src_ref=src, dst_ref=dst, send_sem=pair_send.at[which, t], recv_sem=pair_recv.at[which, t],
            device_id=partner, device_id_type=MESH,
        )

    def dispatch(chunk):
        def act(k, dz, j):
            pltpu.make_async_remote_copy(
                src_ref=send.at[k], dst_ref=recv.at[k], send_sem=out_send, recv_sem=out_recv.at[chunk],
                device_id=at(away(dz, j, 1)), device_id_type=MESH,
            ).start()

        blocks(chunk, act)

    pairs = []
    for chunk in range(len(CHUNKS)):
        dispatch(chunk)
        if chunk == 0:
            pairs = [pair_copy((w_in, w_out)[s], t, s) for t in range(half) for s in (0, 1)]
            for copy in pairs:
                copy.start()
    recv[SELF] = send[SELF]

    eye = lax.broadcasted_iota(jnp.int32, (count, count), 0) == lax.broadcasted_iota(jnp.int32, (count, count), 1)

    def column(row):
        return jnp.sum(jnp.where(eye, row.astype(jnp.float32), 0.0), axis=1, keepdims=True).astype(jnp.int32)

    expert_col, rel_col = column(expert), column(rel)
    logits = jnp.dot(normed[...], router[...], preferred_element_type=jnp.float32)
    powers = jnp.exp(logits - jnp.max(logits, axis=1, keepdims=True))
    lanes = lax.broadcasted_iota(jnp.int32, powers.shape, 1)
    chosen = jnp.sum(jnp.where(lanes == expert_col, powers, 0.0), axis=1, keepdims=True)
    gate[...] = jnp.broadcast_to(chosen / jnp.sum(powers, axis=1, keepdims=True), gate.shape)
    for chunk in range(len(CHUNKS)):
        cols = lax.broadcasted_iota(jnp.int32, (count, CHUNK_ROWS), 1) + chunk * CHUNK_ROWS
        onehot[chunk] = jnp.where(cols == rel_col, 1.0, 0.0).astype(jnp.bfloat16)

    for copy in loads:
        copy.wait()

    def whole(src, dst, chunk, send_sem, recv_sem):
        first = chunk * CHUNK_BLOCKS
        many = CHUNK_BLOCKS - (1 if 0 in CHUNKS[chunk] else 0)
        return pltpu.make_async_remote_copy(
            src_ref=src.at[pl.ds(first, many)], dst_ref=dst.at[pl.ds(first, many)],
            send_sem=send_sem, recv_sem=recv_sem, device_id=partner, device_id_type=MESH,
        )

    for chunk in range(len(CHUNKS)):
        whole(send, recv, chunk, out_send, out_recv.at[chunk]).wait_recv()
        if chunk == 0:
            for copy in pairs:
                copy.wait_recv()
        first = chunk * CHUNK_BLOCKS
        here = recv[first : first + CHUNK_BLOCKS].reshape(CHUNK_ROWS, -1)
        acc[...] = jnp.zeros_like(acc)

        def tile(t, carry):
            hidden = jnp.dot(here, win[t], preferred_element_type=jnp.float32)
            inner = 0.7978845608028654 * (hidden + 0.044715 * (hidden * hidden * hidden))
            hidden = (hidden * (0.5 * (1.0 + jnp.tanh(inner)))).astype(jnp.bfloat16)
            acc[...] += jnp.dot(hidden, wout[t], preferred_element_type=jnp.float32)
            return carry

        lax.fori_loop(0, 2 * half, tile, 0)
        resp[first : first + CHUNK_BLOCKS] = acc[...].reshape(CHUNK_BLOCKS, CAP, -1).astype(jnp.bfloat16)

        def answer(k, dz, j):
            pltpu.make_async_remote_copy(
                src_ref=resp.at[k], dst_ref=back.at[k], send_sem=back_send, recv_sem=back_recv.at[chunk],
                device_id=at(away(dz, j, -1)), device_id_type=MESH,
            ).start()

        blocks(chunk, answer)
    back[SELF] = resp[SELF]

    total = jnp.zeros(values.shape, jnp.float32)
    for chunk in range(len(CHUNKS)):
        whole(resp, back, chunk, back_send, back_recv.at[chunk]).wait_recv()
        first = chunk * CHUNK_BLOCKS
        rows = back[first : first + CHUNK_BLOCKS].reshape(CHUNK_ROWS, -1)
        total = total + jnp.dot(onehot[chunk], rows, preferred_element_type=jnp.float32)
    update[...] = total.astype(jnp.bfloat16)
    mixed[...] = (tokens[...].astype(jnp.float32) + gate[:, :1] * total).astype(jnp.bfloat16)

    for copy in pairs:
        copy.wait_send()
    for chunk in range(len(CHUNKS)):
        whole(send, recv, chunk, out_send, out_recv.at[chunk]).wait_send()
        whole(resp, back, chunk, back_send, back_recv.at[chunk]).wait_send()


def per_device(tokens, ln_gain, router_weight, routes_expert, route_slot, w_in, w_out):
    count, width = tokens.shape
    half = w_in.shape[2] // TILE
    vmem = pl.BlockSpec(memory_space=pltpu.VMEM)
    hbm = pl.BlockSpec(memory_space=pl.ANY)
    blocks = (EXPERTS, CAP, width)
    dma = pltpu.SemaphoreType.DMA
    return pl.pallas_call(
        kernel,
        out_shape=(jax.ShapeDtypeStruct(tokens.shape, jnp.bfloat16),) * 2,
        in_specs=[vmem] * 5 + [hbm] * 2,
        out_specs=(vmem, vmem),
        scratch_shapes=[
            pltpu.VMEM(blocks, jnp.bfloat16),
            pltpu.VMEM(blocks, jnp.bfloat16),
            pltpu.VMEM(blocks, jnp.bfloat16),
            pltpu.VMEM(blocks, jnp.bfloat16),
            pltpu.VMEM((2 * half, width, TILE), jnp.bfloat16),
            pltpu.VMEM((2 * half, TILE, width), jnp.bfloat16),
            pltpu.VMEM((count, width), jnp.bfloat16),
            pltpu.VMEM((CHUNK_ROWS, width), jnp.float32),
            pltpu.VMEM((count, 128), jnp.float32),
            pltpu.VMEM((len(CHUNKS), count, CHUNK_ROWS), jnp.bfloat16),
            dma((2, half)), dma((2, half)), dma((2, half)),
            dma, dma((len(CHUNKS),)), dma, dma((len(CHUNKS),)),
        ],
        compiler_params=pltpu.CompilerParams(
            collective_id=0, has_side_effects=True, vmem_limit_bytes=56 * 1024 * 1024
        ),
    )(
        tokens, ln_gain.reshape(1, -1), router_weight,
        routes_expert.reshape(1, -1), route_slot.reshape(1, -1), w_in, w_out,
    )


def solution(mesh):
    in_specs = (
        P(("dp", "expert"), None),
        P(),
        P(),
        P(("dp", "expert")),
        P(("dp", "expert")),
        P("expert", None, "dp"),
        P("expert", "dp", None),
    )
    out_specs = (P(("dp", "expert"), None), P(("dp", "expert"), None))
    return jax.shard_map(
        per_device, mesh=mesh, in_specs=in_specs, out_specs=out_specs, check_vma=False
    )
```

```python
import functools

import jax
import jax.numpy as jnp
from jax import lax
from jax.experimental import pallas as pl
from jax.experimental.pallas import tpu as pltpu
from jax.sharding import PartitionSpec as P

CAP = 4
ZS, XS, YS = 8, 4, 4
PLANE = XS * YS
EXPERTS = ZS * PLANE
SLOTS = EXPERTS * CAP
CHUNKS = ((3, 5), (2, 6), (4, 0), (1, 7))
ORDER = tuple(dz for pair in CHUNKS for dz in pair)
SELF = ORDER.index(0) * PLANE
CHUNK_BLOCKS = 2 * PLANE
CHUNK_ROWS = CHUNK_BLOCKS * CAP
TILE = 512
MESH = pl.DeviceIdType.MESH


def kernel(
    tokens_in, gain_in, router_in, experts_in, slots_in, w_in, w_out,
    update, gate,
    tokens, gain, router, experts, slots,
    send, recv, resp, back, win, wout, normed, acc, onehot,
    small_sem, load_sem, pair_send, pair_recv, out_send, out_recv, back_send, back_recv,
):
    core = lax.axis_index("dp")
    me = lax.axis_index("expert")
    z, x, y = me // PLANE, lax.rem(me // YS, XS), lax.rem(me, YS)
    half = w_in.shape[2] // TILE

    def at(expert):
        return {"dp": core, "expert": expert}

    def blocks(chunk, sign, act):
        for i, dz in enumerate(CHUNKS[chunk]):
            plane = lax.rem(z + sign * dz + ZS, ZS) * PLANE
            base = (2 * chunk + i) * PLANE
            if dz == 0:
                for dy in range(1, YS):
                    act(base + dy, plane + x * YS + ys[sign][dy])

            def step(dx, carry):
                line = plane + lax.rem(x + sign * dx + XS, XS) * YS
                for dy in range(YS):
                    act(base + dx * YS + dy, line + ys[sign][dy])
                return carry

            lax.fori_loop(1 if dz == 0 else 0, XS, step, 0)

    ys = {sign: [lax.rem(y + sign * dy + YS, YS) for dy in range(YS)] for sign in (1, -1)}

    def greet(k, expert):
        pl.semaphore_signal(barrier, inc=1, device_id=at(expert), device_id_type=MESH)

    small = []
    pieces = ((tokens_in, tokens), (gain_in, gain), (experts_in, experts), (slots_in, slots), (router_in, router))
    for i, (source, target) in enumerate(pieces):
        small.append(pltpu.make_async_copy(source, target, small_sem.at[i]))
        small[-1].start()

    barrier = pltpu.get_barrier_semaphore()
    partner = {"dp": 1 - core, "expert": me}
    pl.semaphore_signal(barrier, inc=1, device_id=partner, device_id_type=MESH)
    for chunk in range(len(CHUNKS)):
        blocks(chunk, 1, greet)

    loads = []
    for t in range(half):
        cols = pl.ds(t * TILE, TILE)
        loads.append(pltpu.make_async_copy(w_in.at[0, :, cols], win.at[t], load_sem.at[0, t]))
        loads.append(pltpu.make_async_copy(w_out.at[0, cols, :], wout.at[t], load_sem.at[1, t]))
    for copy in loads:
        copy.start()

    for copy in small:
        copy.wait()
    values = tokens[...].astype(jnp.float32)
    mean = jnp.mean(values, axis=1, keepdims=True)
    centred = values - mean
    var = jnp.mean(centred * centred, axis=1, keepdims=True)
    normed[...] = (centred * lax.rsqrt(var + 1e-06) * gain[...]).astype(jnp.bfloat16)

    expert = experts[...]
    slot = slots[...]
    dz = (expert // PLANE - z) & (ZS - 1)
    dx = ((expert // YS) % XS - x) & (XS - 1)
    dy = (expert % YS - y) & (YS - 1)
    place = jnp.zeros_like(dz)
    for i, d in enumerate(ORDER):
        place = jnp.where(dz == d, i, place)
    rel = ((place * PLANE) + dx * YS + dy) * CAP + slot
    rel = jnp.where(slot >= 0, rel, -1)
    count = rel.shape[1]
    for chunk in range(len(CHUNKS)):
        rows = lax.broadcasted_iota(jnp.int32, (CHUNK_ROWS, count), 0) + chunk * CHUNK_ROWS
        pick = jnp.where(rows == rel, 1.0, 0.0).astype(jnp.bfloat16)
        picked = jnp.dot(pick, normed[...], preferred_element_type=jnp.float32)
        first = chunk * CHUNK_BLOCKS
        send[first : first + CHUNK_BLOCKS] = picked.reshape(CHUNK_BLOCKS, CAP, -1).astype(jnp.bfloat16)

    pl.semaphore_wait(barrier, EXPERTS)

    def pair_copy(w, t, which):
        dst = (win, wout)[which].at[half + t]
        src = w.at[0, :, pl.ds(t * TILE, TILE)] if which == 0 else w.at[0, pl.ds(t * TILE, TILE), :]
        return pltpu.make_async_remote_copy(
            src_ref=src, dst_ref=dst, send_sem=pair_send.at[which, t], recv_sem=pair_recv.at[which, t],
            device_id=partner, device_id_type=MESH,
        )

    def dispatch(chunk):
        def act(k, expert):
            pltpu.make_async_remote_copy(
                src_ref=send.at[k], dst_ref=recv.at[k], send_sem=out_send, recv_sem=out_recv.at[chunk],
                device_id=at(expert), device_id_type=MESH,
            ).start()

        blocks(chunk, 1, act)

    pairs = []
    for chunk in range(len(CHUNKS)):
        dispatch(chunk)
        if chunk == 0:
            pairs = [pair_copy((w_in, w_out)[s], t, s) for t in range(half) for s in (0, 1)]
            for copy in pairs:
                copy.start()
    recv[SELF] = send[SELF]

    eye = lax.broadcasted_iota(jnp.int32, (count, count), 0) == lax.broadcasted_iota(jnp.int32, (count, count), 1)

    def column(row):
        return jnp.sum(jnp.where(eye, row.astype(jnp.float32), 0.0), axis=1, keepdims=True).astype(jnp.int32)

    expert_col, rel_col = column(expert), column(rel)
    logits = jnp.dot(normed[...], router[...], preferred_element_type=jnp.float32)
    powers = jnp.exp(logits - jnp.max(logits, axis=1, keepdims=True))
    lanes = lax.broadcasted_iota(jnp.int32, powers.shape, 1)
    chosen = jnp.sum(jnp.where(lanes == expert_col, powers, 0.0), axis=1, keepdims=True)
    gate[...] = jnp.broadcast_to(chosen / jnp.sum(powers, axis=1, keepdims=True), gate.shape)
    for chunk in range(len(CHUNKS)):
        cols = lax.broadcasted_iota(jnp.int32, (count, CHUNK_ROWS), 1) + chunk * CHUNK_ROWS
        onehot[chunk] = jnp.where(cols == rel_col, 1.0, 0.0).astype(jnp.bfloat16)

    for copy in loads:
        copy.wait()

    def whole(src, dst, chunk, send_sem, recv_sem):
        first = chunk * CHUNK_BLOCKS
        many = CHUNK_BLOCKS - (1 if 0 in CHUNKS[chunk] else 0)
        return pltpu.make_async_remote_copy(
            src_ref=src.at[pl.ds(first, many)], dst_ref=dst.at[pl.ds(first, many)],
            send_sem=send_sem, recv_sem=recv_sem, device_id=partner, device_id_type=MESH,
        )

    for chunk in range(len(CHUNKS)):
        whole(send, recv, chunk, out_send, out_recv.at[chunk]).wait_recv()
        if chunk == 0:
            for copy in pairs:
                copy.wait_recv()
        first = chunk * CHUNK_BLOCKS
        here = recv[first : first + CHUNK_BLOCKS].reshape(CHUNK_ROWS, -1)
        acc[...] = jnp.zeros_like(acc)

        def tile(t, carry):
            hidden = jnp.dot(here, win[t], preferred_element_type=jnp.float32)
            inner = 0.7978845608028654 * (hidden + 0.044715 * (hidden * hidden * hidden))
            hidden = (hidden * (0.5 * (1.0 + jnp.tanh(inner)))).astype(jnp.bfloat16)
            acc[...] += jnp.dot(hidden, wout[t], preferred_element_type=jnp.float32)
            return carry

        lax.fori_loop(0, 2 * half, tile, 0)
        resp[first : first + CHUNK_BLOCKS] = acc[...].reshape(CHUNK_BLOCKS, CAP, -1).astype(jnp.bfloat16)

        def answer(k, expert):
            pltpu.make_async_remote_copy(
                src_ref=resp.at[k], dst_ref=back.at[k], send_sem=back_send, recv_sem=back_recv.at[chunk],
                device_id=at(expert), device_id_type=MESH,
            ).start()

        blocks(chunk, -1, answer)
    back[SELF] = resp[SELF]

    total = jnp.zeros(values.shape, jnp.float32)
    for chunk in range(len(CHUNKS)):
        whole(resp, back, chunk, back_send, back_recv.at[chunk]).wait_recv()
        first = chunk * CHUNK_BLOCKS
        rows = back[first : first + CHUNK_BLOCKS].reshape(CHUNK_ROWS, -1)
        total = total + jnp.dot(onehot[chunk], rows, preferred_element_type=jnp.float32)
    update[...] = total.astype(jnp.bfloat16)

    for copy in pairs:
        copy.wait_send()
    for chunk in range(len(CHUNKS)):
        whole(send, recv, chunk, out_send, out_recv.at[chunk]).wait_send()
        whole(resp, back, chunk, back_send, back_recv.at[chunk]).wait_send()


def finish(tokens, gate, total, mixed, update):
    update[...] = total[...]
    values = tokens[...].astype(jnp.float32)
    mixed[...] = (values + gate[:, :1] * total[...].astype(jnp.float32)).astype(jnp.bfloat16)


def per_device(tokens, ln_gain, router_weight, routes_expert, route_slot, w_in, w_out):
    count, width = tokens.shape
    half = w_in.shape[2] // TILE
    vmem = pl.BlockSpec(memory_space=pltpu.VMEM)
    hbm = pl.BlockSpec(memory_space=pltpu.MemorySpace.HBM)
    blocks = (EXPERTS, CAP, width)
    dma = pltpu.SemaphoreType.DMA
    shape = jax.ShapeDtypeStruct(tokens.shape, jnp.bfloat16)
    total, gate = pl.pallas_call(
        kernel,
        out_shape=(pltpu.VMEM(tokens.shape, jnp.bfloat16), pltpu.VMEM((count, 128), jnp.float32)),
        in_specs=[hbm] * 7,
        out_specs=(vmem, vmem),
        scratch_shapes=[
            pltpu.VMEM(tokens.shape, jnp.bfloat16),
            pltpu.VMEM((1, width), jnp.float32),
            pltpu.VMEM(router_weight.shape, jnp.bfloat16),
            pltpu.VMEM((1, count), jnp.int32),
            pltpu.VMEM((1, count), jnp.int32),
            pltpu.VMEM(blocks, jnp.bfloat16),
            pltpu.VMEM(blocks, jnp.bfloat16),
            pltpu.VMEM(blocks, jnp.bfloat16),
            pltpu.VMEM(blocks, jnp.bfloat16),
            pltpu.VMEM((2 * half, width, TILE), jnp.bfloat16),
            pltpu.VMEM((2 * half, TILE, width), jnp.bfloat16),
            pltpu.VMEM((count, width), jnp.bfloat16),
            pltpu.VMEM((CHUNK_ROWS, width), jnp.float32),
            pltpu.VMEM((len(CHUNKS), count, CHUNK_ROWS), jnp.bfloat16),
            dma((5,)), dma((2, half)), dma((2, half)), dma((2, half)),
            dma, dma((len(CHUNKS),)), dma, dma((len(CHUNKS),)),
        ],
        compiler_params=pltpu.CompilerParams(
            collective_id=0, has_side_effects=True, vmem_limit_bytes=32 * 1024 * 1024
        ),
    )(
        *(
            pltpu.with_memory_space_constraint(value, pltpu.MemorySpace.HBM)
            for value in (
                tokens, ln_gain.reshape(1, -1), router_weight,
                routes_expert.reshape(1, -1), route_slot.reshape(1, -1), w_in, w_out,
            )
        )
    )
    return pl.pallas_call(
        finish,
        out_shape=(shape, shape),
        in_specs=[vmem] * 3,
        out_specs=(vmem, vmem),
        compiler_params=pltpu.CompilerParams(vmem_limit_bytes=8 * 1024 * 1024),
    )(tokens, gate, total)


def solution(mesh):
    in_specs = (
        P(("dp", "expert"), None),
        P(),
        P(),
        P(("dp", "expert")),
        P(("dp", "expert")),
        P("expert", None, "dp"),
        P("expert", "dp", None),
    )
    out_specs = (P(("dp", "expert"), None), P(("dp", "expert"), None))
    return jax.shard_map(
        per_device, mesh=mesh, in_specs=in_specs, out_specs=out_specs, check_vma=False
    )
```

```python
import functools

import jax
import jax.numpy as jnp
from jax import lax
from jax.experimental import pallas as pl
from jax.experimental.pallas import tpu as pltpu
from jax.sharding import PartitionSpec as P

CAP = 4
ZS, XS, YS = 8, 4, 4
PLANE = XS * YS
EXPERTS = ZS * PLANE
SLOTS = EXPERTS * CAP
CHUNKS = ((2, 6), (4, 0), (3, 5), (1, 7))
ORDER = tuple(dz for pair in CHUNKS for dz in pair)
SELF = ORDER.index(0) * PLANE
CHUNK_BLOCKS = 2 * PLANE
CHUNK_ROWS = CHUNK_BLOCKS * CAP
TILE = 512
MESH = pl.DeviceIdType.MESH


def kernel(
    tokens_in, gain_in, router_in, experts_in, slots_in, w_in, w_out,
    update, gate,
    tokens, gain, router, experts, slots,
    send, recv, resp, back, win, wout, normed, acc, onehot,
    small_sem, load_sem, pair_send, pair_recv, out_send, out_recv, back_send, back_recv,
):
    core = lax.axis_index("dp")
    me = lax.axis_index("expert")
    z, x, y = me // PLANE, lax.rem(me // YS, XS), lax.rem(me, YS)
    half = w_in.shape[2] // TILE

    def at(expert):
        return {"dp": core, "expert": expert}

    def blocks(chunk, sign, act, far_first=False):
        for i, dz in enumerate(CHUNKS[chunk]):
            plane = lax.rem(z + sign * dz + ZS, ZS) * PLANE
            base = (2 * chunk + i) * PLANE
            if dz == 0:
                for dy in range(1, YS):
                    act(base + dy, plane + x * YS + ys[sign][dy])

            def step(s, carry):
                t = XS - 1 - s
                dx = t + t // 2 - 2 * (t // 3) if far_first else s
                line = plane + lax.rem(x + sign * dx + XS, XS) * YS
                for dy in (2, 1, 3, 0) if far_first else range(YS):
                    act(base + dx * YS + dy, line + ys[sign][dy])
                return carry

            first = 1 if dz == 0 else 0
            lax.fori_loop(0 if far_first else first, XS - first if far_first else XS, step, 0)

    ys = {sign: [lax.rem(y + sign * dy + YS, YS) for dy in range(YS)] for sign in (1, -1)}

    def greet(k, expert):
        pl.semaphore_signal(barrier, inc=1, device_id=at(expert), device_id_type=MESH)

    small = []
    pieces = ((tokens_in, tokens), (gain_in, gain), (experts_in, experts), (slots_in, slots), (router_in, router))
    for i, (source, target) in enumerate(pieces):
        small.append(pltpu.make_async_copy(source, target, small_sem.at[i]))
        small[-1].start()

    barrier = pltpu.get_barrier_semaphore()
    partner = {"dp": 1 - core, "expert": me}
    pl.semaphore_signal(barrier, inc=1, device_id=partner, device_id_type=MESH)
    for chunk in range(len(CHUNKS)):
        blocks((1, 2, 0, 3)[chunk], 1, greet, True)

    loads = []
    for t in range(half):
        cols = pl.ds(t * TILE, TILE)
        loads.append(pltpu.make_async_copy(w_in.at[0, :, cols], win.at[t], load_sem.at[0, t]))
        loads.append(pltpu.make_async_copy(w_out.at[0, cols, :], wout.at[t], load_sem.at[1, t]))
    for copy in loads:
        copy.start()

    for copy in small:
        copy.wait()
    values = tokens[...].astype(jnp.float32)
    mean = jnp.mean(values, axis=1, keepdims=True)
    centred = values - mean
    var = jnp.mean(centred * centred, axis=1, keepdims=True)
    normed[...] = (centred * lax.rsqrt(var + 1e-06) * gain[...]).astype(jnp.bfloat16)

    expert = experts[...]
    slot = slots[...]
    dz = (expert // PLANE - z) & (ZS - 1)
    dx = ((expert // YS) % XS - x) & (XS - 1)
    dy = (expert % YS - y) & (YS - 1)
    place = jnp.zeros_like(dz)
    for i, d in enumerate(ORDER):
        place = jnp.where(dz == d, i, place)
    rel = ((place * PLANE) + dx * YS + dy) * CAP + slot
    rel = jnp.where(slot >= 0, rel, -1)
    count = rel.shape[1]
    for chunk in range(len(CHUNKS)):
        rows = lax.broadcasted_iota(jnp.int32, (CHUNK_ROWS, count), 0) + chunk * CHUNK_ROWS
        pick = jnp.where(rows == rel, 1.0, 0.0).astype(jnp.bfloat16)
        picked = jnp.dot(pick, normed[...], preferred_element_type=jnp.float32)
        first = chunk * CHUNK_BLOCKS
        send[first : first + CHUNK_BLOCKS] = picked.reshape(CHUNK_BLOCKS, CAP, -1).astype(jnp.bfloat16)

    pl.semaphore_wait(barrier, EXPERTS)

    def pair_copy(w, t, which):
        dst = (win, wout)[which].at[half + t]
        src = w.at[0, :, pl.ds(t * TILE, TILE)] if which == 0 else w.at[0, pl.ds(t * TILE, TILE), :]
        return pltpu.make_async_remote_copy(
            src_ref=src, dst_ref=dst, send_sem=pair_send.at[which, t], recv_sem=pair_recv.at[which, t],
            device_id=partner, device_id_type=MESH,
        )

    def dispatch(chunk):
        def act(k, expert):
            pltpu.make_async_remote_copy(
                src_ref=send.at[k], dst_ref=recv.at[k], send_sem=out_send, recv_sem=out_recv.at[chunk],
                device_id=at(expert), device_id_type=MESH,
            ).start()

        blocks(chunk, 1, act)

    pairs = []
    for chunk in range(len(CHUNKS)):
        dispatch(chunk)
        if chunk == 0:
            pairs = [pair_copy((w_in, w_out)[s], t, s) for t in range(half) for s in (0, 1)]
            for copy in pairs:
                copy.start()
    recv[SELF] = send[SELF]

    eye = lax.broadcasted_iota(jnp.int32, (count, count), 0) == lax.broadcasted_iota(jnp.int32, (count, count), 1)

    def column(row):
        return jnp.sum(jnp.where(eye, row.astype(jnp.float32), 0.0), axis=1, keepdims=True).astype(jnp.int32)

    expert_col, rel_col = column(expert), column(rel)
    logits = jnp.dot(normed[...], router[...], preferred_element_type=jnp.float32)
    powers = jnp.exp(logits - jnp.max(logits, axis=1, keepdims=True))
    lanes = lax.broadcasted_iota(jnp.int32, powers.shape, 1)
    chosen = jnp.sum(jnp.where(lanes == expert_col, powers, 0.0), axis=1, keepdims=True)
    gate[...] = jnp.broadcast_to(chosen / jnp.sum(powers, axis=1, keepdims=True), gate.shape)
    for chunk in range(len(CHUNKS)):
        cols = lax.broadcasted_iota(jnp.int32, (count, CHUNK_ROWS), 1) + chunk * CHUNK_ROWS
        onehot[chunk] = jnp.where(cols == rel_col, 1.0, 0.0).astype(jnp.bfloat16)

    for copy in loads:
        copy.wait()

    def whole(src, dst, chunk, send_sem, recv_sem):
        first = chunk * CHUNK_BLOCKS
        many = CHUNK_BLOCKS - (1 if 0 in CHUNKS[chunk] else 0)
        return pltpu.make_async_remote_copy(
            src_ref=src.at[pl.ds(first, many)], dst_ref=dst.at[pl.ds(first, many)],
            send_sem=send_sem, recv_sem=recv_sem, device_id=partner, device_id_type=MESH,
        )

    for chunk in range(len(CHUNKS)):
        whole(send, recv, chunk, out_send, out_recv.at[chunk]).wait_recv()
        if chunk == 0:
            for copy in pairs:
                copy.wait_recv()
        first = chunk * CHUNK_BLOCKS
        here = recv[first : first + CHUNK_BLOCKS].reshape(CHUNK_ROWS, -1)
        acc[...] = jnp.zeros_like(acc)

        def tile(t, carry):
            hidden = jnp.dot(here, win[t], preferred_element_type=jnp.float32)
            inner = 0.7978845608028654 * (hidden + 0.044715 * (hidden * hidden * hidden))
            hidden = (hidden * (0.5 * (1.0 + jnp.tanh(inner)))).astype(jnp.bfloat16)
            acc[...] += jnp.dot(hidden, wout[t], preferred_element_type=jnp.float32)
            return carry

        lax.fori_loop(0, 2 * half, tile, 0)
        resp[first : first + CHUNK_BLOCKS] = acc[...].reshape(CHUNK_BLOCKS, CAP, -1).astype(jnp.bfloat16)

        def answer(k, expert):
            pltpu.make_async_remote_copy(
                src_ref=resp.at[k], dst_ref=back.at[k], send_sem=back_send, recv_sem=back_recv.at[chunk],
                device_id=at(expert), device_id_type=MESH,
            ).start()

        blocks(chunk, -1, answer, True)
    back[SELF] = resp[SELF]

    total = jnp.zeros(values.shape, jnp.float32)
    for chunk in range(len(CHUNKS)):
        whole(resp, back, chunk, back_send, back_recv.at[chunk]).wait_recv()
        first = chunk * CHUNK_BLOCKS
        rows = back[first : first + CHUNK_BLOCKS].reshape(CHUNK_ROWS, -1)
        total = total + jnp.dot(onehot[chunk], rows, preferred_element_type=jnp.float32)
    update[...] = total.astype(jnp.bfloat16)

    for copy in pairs:
        copy.wait_send()
    for chunk in range(len(CHUNKS)):
        whole(send, recv, chunk, out_send, out_recv.at[chunk]).wait_send()
        whole(resp, back, chunk, back_send, back_recv.at[chunk]).wait_send()


def finish(tokens, gate, total, mixed, update):
    update[...] = total[...]
    values = tokens[...].astype(jnp.float32)
    mixed[...] = (values + gate[:, :1] * total[...].astype(jnp.float32)).astype(jnp.bfloat16)


def per_device(tokens, ln_gain, router_weight, routes_expert, route_slot, w_in, w_out):
    count, width = tokens.shape
    half = w_in.shape[2] // TILE
    vmem = pl.BlockSpec(memory_space=pltpu.VMEM)
    hbm = pl.BlockSpec(memory_space=pltpu.MemorySpace.HBM)
    blocks = (EXPERTS, CAP, width)
    dma = pltpu.SemaphoreType.DMA
    shape = jax.ShapeDtypeStruct(tokens.shape, jnp.bfloat16)
    total, gate = pl.pallas_call(
        kernel,
        out_shape=(pltpu.VMEM(tokens.shape, jnp.bfloat16), pltpu.VMEM((count, 128), jnp.float32)),
        in_specs=[hbm] * 7,
        out_specs=(vmem, vmem),
        scratch_shapes=[
            pltpu.VMEM(tokens.shape, jnp.bfloat16),
            pltpu.VMEM((1, width), jnp.float32),
            pltpu.VMEM(router_weight.shape, jnp.bfloat16),
            pltpu.VMEM((1, count), jnp.int32),
            pltpu.VMEM((1, count), jnp.int32),
            pltpu.VMEM(blocks, jnp.bfloat16),
            pltpu.VMEM(blocks, jnp.bfloat16),
            pltpu.VMEM(blocks, jnp.bfloat16),
            pltpu.VMEM(blocks, jnp.bfloat16),
            pltpu.VMEM((2 * half, width, TILE), jnp.bfloat16),
            pltpu.VMEM((2 * half, TILE, width), jnp.bfloat16),
            pltpu.VMEM((count, width), jnp.bfloat16),
            pltpu.VMEM((CHUNK_ROWS, width), jnp.float32),
            pltpu.VMEM((len(CHUNKS), count, CHUNK_ROWS), jnp.bfloat16),
            dma((5,)), dma((2, half)), dma((2, half)), dma((2, half)),
            dma, dma((len(CHUNKS),)), dma, dma((len(CHUNKS),)),
        ],
        compiler_params=pltpu.CompilerParams(
            collective_id=0, has_side_effects=True, vmem_limit_bytes=32 * 1024 * 1024
        ),
    )(
        *(
            pltpu.with_memory_space_constraint(value, pltpu.MemorySpace.HBM)
            for value in (
                tokens, ln_gain.reshape(1, -1), router_weight,
                routes_expert.reshape(1, -1), route_slot.reshape(1, -1), w_in, w_out,
            )
        )
    )
    return pl.pallas_call(
        finish,
        out_shape=(shape, shape),
        grid=(2,),
        in_specs=[pl.BlockSpec((count // 2, n), lambda i: (i, 0)) for n in (width, 128, width)],
        out_specs=(pl.BlockSpec((count // 2, width), lambda i: (i, 0)),) * 2,
        compiler_params=pltpu.CompilerParams(vmem_limit_bytes=8 * 1024 * 1024),
    )(tokens, gate, total)


def solution(mesh):
    in_specs = (
        P(("dp", "expert"), None),
        P(),
        P(),
        P(("dp", "expert")),
        P(("dp", "expert")),
        P("expert", None, "dp"),
        P("expert", "dp", None),
    )
    out_specs = (P(("dp", "expert"), None), P(("dp", "expert"), None))
    return jax.shard_map(
        per_device, mesh=mesh, in_specs=in_specs, out_specs=out_specs, check_vma=False
    )
```

```python
import functools

import jax
import jax.numpy as jnp
from jax import lax
from jax.experimental import pallas as pl
from jax.experimental.pallas import tpu as pltpu
from jax.sharding import PartitionSpec as P

CAP = 4
ZS, XS, YS = 8, 4, 4
PLANE = XS * YS
EXPERTS = ZS * PLANE
SLOTS = EXPERTS * CAP
CHUNKS = ((2, 6), (4, 0), (3, 5), (1, 7))
ORDER = tuple(dz for pair in CHUNKS for dz in pair)
SELF = ORDER.index(0) * PLANE
SELF_CHUNK = ORDER.index(0) // 2
CHUNK_BLOCKS = 2 * PLANE
CHUNK_ROWS = CHUNK_BLOCKS * CAP
TILE = 512
MESH = pl.DeviceIdType.MESH


def kernel(
    tokens_in, gain_in, router_in, experts_in, slots_in, w_in, w_out,
    update, gate,
    tokens, gain, router, experts, slots,
    send, recv, resp, back, win, wout, normed, acc, onehot,
    ready, small_sem, load_sem, pair_send, pair_recv, out_send, out_recv, back_send, back_recv,
):
    core = lax.axis_index("dp")
    me = lax.axis_index("expert")
    z, x, y = me // PLANE, lax.rem(me // YS, XS), lax.rem(me, YS)
    half = w_in.shape[2] // TILE

    def at(expert):
        return {"dp": core, "expert": expert}

    def blocks(chunk, sign, act, far_first=False, column=True, only=tuple(range(ZS))):
        for i, dz in enumerate(CHUNKS[chunk]):
            if dz not in only:
                continue
            plane = lax.rem(z + sign * dz + ZS, ZS) * PLANE
            base = (2 * chunk + i) * PLANE
            whole_column = column and dz != 0
            if not column and dz != 0:
                pl.semaphore_wait(ready.at[dz], 1)
            if not whole_column:
                for dy in range(1, YS):
                    act(base + dy, plane + x * YS + ys[sign][dy])

            def step(s, carry):
                t = XS - 1 - s
                dx = t + t // 2 - 2 * (t // 3) if far_first else s
                line = plane + lax.rem(x + sign * dx + XS, XS) * YS
                for dy in (2, 1, 3, 0) if far_first else range(YS):
                    act(base + dx * YS + dy, line + ys[sign][dy])
                return carry

            first = 0 if whole_column else 1
            lax.fori_loop(0 if far_first else first, XS - first if far_first else XS, step, 0)

    columns = tuple((ORDER.index(dz) * PLANE, dz, lax.rem(z + dz, ZS) * PLANE + x * YS + y) for dz in ORDER if dz)
    ys = {sign: [lax.rem(y + sign * dy + YS, YS) for dy in range(YS)] for sign in (1, -1)}

    def greet(k, expert):
        pl.semaphore_signal(barrier, inc=1, device_id=at(expert), device_id_type=MESH)

    small = []
    pieces = ((tokens_in, tokens), (gain_in, gain), (experts_in, experts), (slots_in, slots), (router_in, router))
    for i, (source, target) in enumerate(pieces):
        small.append(pltpu.make_async_copy(source, target, small_sem.at[i]))
        small[-1].start()

    barrier = pltpu.get_barrier_semaphore()
    partner = {"dp": 1 - core, "expert": me}
    pl.semaphore_signal(barrier, inc=1, device_id=partner, device_id_type=MESH)
    for k, dz, peer in columns:
        greet(k, peer)
    blocks(SELF_CHUNK, 1, greet, True, False, (0,))

    loads = []
    for t in range(half):
        cols = pl.ds(t * TILE, TILE)
        loads.append(pltpu.make_async_copy(w_in.at[0, :, cols], win.at[t], load_sem.at[0, t]))
        loads.append(pltpu.make_async_copy(w_out.at[0, cols, :], wout.at[t], load_sem.at[1, t]))
    for copy in loads:
        copy.start()

    for copy in small:
        copy.wait()
    values = tokens[...].astype(jnp.float32)
    mean = jnp.mean(values, axis=1, keepdims=True)
    centred = values - mean
    var = jnp.mean(centred * centred, axis=1, keepdims=True)
    normed[...] = (centred * lax.rsqrt(var + 1e-06) * gain[...]).astype(jnp.bfloat16)

    expert = experts[...]
    slot = slots[...]
    dz = (expert // PLANE - z) & (ZS - 1)
    dx = ((expert // YS) % XS - x) & (XS - 1)
    dy = (expert % YS - y) & (YS - 1)
    place = jnp.zeros_like(dz)
    for i, d in enumerate(ORDER):
        place = jnp.where(dz == d, i, place)
    rel = ((place * PLANE) + dx * YS + dy) * CAP + slot
    rel = jnp.where(slot >= 0, rel, -1)
    count = rel.shape[1]
    for chunk in range(len(CHUNKS)):
        rows = lax.broadcasted_iota(jnp.int32, (CHUNK_ROWS, count), 0) + chunk * CHUNK_ROWS
        pick = jnp.where(rows == rel, 1.0, 0.0).astype(jnp.bfloat16)
        picked = jnp.dot(pick, normed[...], preferred_element_type=jnp.float32)
        first = chunk * CHUNK_BLOCKS
        send[first : first + CHUNK_BLOCKS] = picked.reshape(CHUNK_BLOCKS, CAP, -1).astype(jnp.bfloat16)

    pl.semaphore_wait(barrier, len(columns) + PLANE)
    for k, dz, peer in columns:
        pl.semaphore_signal(ready.at[ZS - dz], inc=1, device_id=at(peer), device_id_type=MESH)

    def pair_copy(w, t, which):
        dst = (win, wout)[which].at[half + t]
        src = w.at[0, :, pl.ds(t * TILE, TILE)] if which == 0 else w.at[0, pl.ds(t * TILE, TILE), :]
        return pltpu.make_async_remote_copy(
            src_ref=src, dst_ref=dst, send_sem=pair_send.at[which, t], recv_sem=pair_recv.at[which, t],
            device_id=partner, device_id_type=MESH,
        )

    def dispatch(chunk):
        def act(k, expert):
            pltpu.make_async_remote_copy(
                src_ref=send.at[k], dst_ref=recv.at[k], send_sem=out_send, recv_sem=out_recv.at[chunk],
                device_id=at(expert), device_id_type=MESH,
            ).start()

        return act

    for k, dz, peer in columns:
        dispatch(ORDER.index(dz) // 2)(k, peer)
    pairs = []
    for chunk in range(len(CHUNKS)):
        blocks(chunk, 1, dispatch(chunk), column=False)
        if chunk == 0:
            pairs = [pair_copy((w_in, w_out)[s], t, s) for t in range(half) for s in (0, 1)]
            for copy in pairs:
                copy.start()
    recv[SELF] = send[SELF]

    eye = lax.broadcasted_iota(jnp.int32, (count, count), 0) == lax.broadcasted_iota(jnp.int32, (count, count), 1)

    def column(row):
        return jnp.sum(jnp.where(eye, row.astype(jnp.float32), 0.0), axis=1, keepdims=True).astype(jnp.int32)

    expert_col, rel_col = column(expert), column(rel)
    logits = jnp.dot(normed[...], router[...], preferred_element_type=jnp.float32)
    powers = jnp.exp(logits - jnp.max(logits, axis=1, keepdims=True))
    lanes = lax.broadcasted_iota(jnp.int32, powers.shape, 1)
    chosen = jnp.sum(jnp.where(lanes == expert_col, powers, 0.0), axis=1, keepdims=True)
    gate[...] = jnp.broadcast_to(chosen / jnp.sum(powers, axis=1, keepdims=True), gate.shape)
    for chunk in range(len(CHUNKS)):
        cols = lax.broadcasted_iota(jnp.int32, (count, CHUNK_ROWS), 1) + chunk * CHUNK_ROWS
        onehot[chunk] = jnp.where(cols == rel_col, 1.0, 0.0).astype(jnp.bfloat16)

    for copy in loads:
        copy.wait()

    def whole(src, dst, chunk, send_sem, recv_sem):
        first = chunk * CHUNK_BLOCKS
        many = CHUNK_BLOCKS - (1 if 0 in CHUNKS[chunk] else 0)
        return pltpu.make_async_remote_copy(
            src_ref=src.at[pl.ds(first, many)], dst_ref=dst.at[pl.ds(first, many)],
            send_sem=send_sem, recv_sem=recv_sem, device_id=partner, device_id_type=MESH,
        )

    for chunk in range(len(CHUNKS)):
        whole(send, recv, chunk, out_send, out_recv.at[chunk]).wait_recv()
        first = chunk * CHUNK_BLOCKS
        here = recv[first : first + CHUNK_BLOCKS].reshape(CHUNK_ROWS, -1)
        acc[...] = jnp.zeros_like(acc)

        def tile(t, carry):
            hidden = jnp.dot(here, win[t], preferred_element_type=jnp.float32)
            inner = 0.7978845608028654 * (hidden + 0.044715 * (hidden * hidden * hidden))
            hidden = (hidden * (0.5 * (1.0 + jnp.tanh(inner)))).astype(jnp.bfloat16)
            acc[...] += jnp.dot(hidden, wout[t], preferred_element_type=jnp.float32)
            return carry

        if chunk == 0:
            lax.fori_loop(0, half, tile, 0)
            for t in range(half):
                for copy in pairs[2 * t : 2 * t + 2]:
                    copy.wait_recv()
                tile(half + t, 0)
        else:
            lax.fori_loop(0, 2 * half, tile, 0)
        resp[first : first + CHUNK_BLOCKS] = acc[...].reshape(CHUNK_BLOCKS, CAP, -1).astype(jnp.bfloat16)

        def answer(k, expert):
            pltpu.make_async_remote_copy(
                src_ref=resp.at[k], dst_ref=back.at[k], send_sem=back_send, recv_sem=back_recv.at[chunk],
                device_id=at(expert), device_id_type=MESH,
            ).start()

        blocks(chunk, -1, answer, True)
    back[SELF] = resp[SELF]

    total = jnp.zeros(values.shape, jnp.float32)
    for chunk in range(len(CHUNKS)):
        whole(resp, back, chunk, back_send, back_recv.at[chunk]).wait_recv()
        first = chunk * CHUNK_BLOCKS
        rows = back[first : first + CHUNK_BLOCKS].reshape(CHUNK_ROWS, -1)
        total = total + jnp.dot(onehot[chunk], rows, preferred_element_type=jnp.float32)
    update[...] = total.astype(jnp.bfloat16)

    for copy in pairs:
        copy.wait_send()
    for chunk in range(len(CHUNKS)):
        whole(send, recv, chunk, out_send, out_recv.at[chunk]).wait_send()
        whole(resp, back, chunk, back_send, back_recv.at[chunk]).wait_send()


def finish(tokens, gate, total, mixed, update):
    update[...] = total[...]
    values = tokens[...].astype(jnp.float32)
    mixed[...] = (values + gate[:, :1] * total[...].astype(jnp.float32)).astype(jnp.bfloat16)


def per_device(tokens, ln_gain, router_weight, routes_expert, route_slot, w_in, w_out):
    count, width = tokens.shape
    half = w_in.shape[2] // TILE
    vmem = pl.BlockSpec(memory_space=pltpu.VMEM)
    hbm = pl.BlockSpec(memory_space=pltpu.MemorySpace.HBM)
    blocks = (EXPERTS, CAP, width)
    dma = pltpu.SemaphoreType.DMA
    shape = jax.ShapeDtypeStruct(tokens.shape, jnp.bfloat16)
    total, gate = pl.pallas_call(
        kernel,
        out_shape=(pltpu.VMEM(tokens.shape, jnp.bfloat16), pltpu.VMEM((count, 128), jnp.float32)),
        in_specs=[hbm] * 7,
        out_specs=(vmem, vmem),
        scratch_shapes=[
            pltpu.VMEM(tokens.shape, jnp.bfloat16),
            pltpu.VMEM((1, width), jnp.float32),
            pltpu.VMEM(router_weight.shape, jnp.bfloat16),
            pltpu.VMEM((1, count), jnp.int32),
            pltpu.VMEM((1, count), jnp.int32),
            pltpu.VMEM(blocks, jnp.bfloat16),
            pltpu.VMEM(blocks, jnp.bfloat16),
            pltpu.VMEM(blocks, jnp.bfloat16),
            pltpu.VMEM(blocks, jnp.bfloat16),
            pltpu.VMEM((2 * half, width, TILE), jnp.bfloat16),
            pltpu.VMEM((2 * half, TILE, width), jnp.bfloat16),
            pltpu.VMEM((count, width), jnp.bfloat16),
            pltpu.VMEM((CHUNK_ROWS, width), jnp.float32),
            pltpu.VMEM((len(CHUNKS), count, CHUNK_ROWS), jnp.bfloat16),
            pltpu.SemaphoreType.REGULAR((ZS,)), dma((5,)), dma((2, half)), dma((2, half)), dma((2, half)),
            dma, dma((len(CHUNKS),)), dma, dma((len(CHUNKS),)),
        ],
        compiler_params=pltpu.CompilerParams(
            collective_id=0, has_side_effects=True, vmem_limit_bytes=32 * 1024 * 1024
        ),
    )(
        *(
            pltpu.with_memory_space_constraint(value, pltpu.MemorySpace.HBM)
            for value in (
                tokens, ln_gain.reshape(1, -1), router_weight,
                routes_expert.reshape(1, -1), route_slot.reshape(1, -1), w_in, w_out,
            )
        )
    )
    return pl.pallas_call(
        finish,
        out_shape=(shape, shape),
        grid=(2,),
        in_specs=[pl.BlockSpec((count // 2, n), lambda i: (i, 0)) for n in (width, 128, width)],
        out_specs=(pl.BlockSpec((count // 2, width), lambda i: (i, 0)),) * 2,
        compiler_params=pltpu.CompilerParams(vmem_limit_bytes=8 * 1024 * 1024),
    )(tokens, gate, total)


def solution(mesh):
    in_specs = (
        P(("dp", "expert"), None),
        P(),
        P(),
        P(("dp", "expert")),
        P(("dp", "expert")),
        P("expert", None, "dp"),
        P("expert", "dp", None),
    )
    out_specs = (P(("dp", "expert"), None), P(("dp", "expert"), None))
    return jax.shard_map(
        per_device, mesh=mesh, in_specs=in_specs, out_specs=out_specs, check_vma=False
    )
```

```python
import functools

import jax
import jax.numpy as jnp
from jax import lax
from jax.experimental import pallas as pl
from jax.experimental.pallas import tpu as pltpu
from jax.sharding import PartitionSpec as P

CAP = 4
ZS, XS, YS = 8, 4, 4
PLANE = XS * YS
EXPERTS = ZS * PLANE
SLOTS = EXPERTS * CAP
CHUNKS = ((2, 6), (3, 5), (0, 4), (1, 7))
ORDER = tuple(dz for pair in CHUNKS for dz in pair)
SELF = ORDER.index(0) * PLANE
SELF_CHUNK = ORDER.index(0) // 2
CHUNK_BLOCKS = 2 * PLANE
CHUNK_ROWS = CHUNK_BLOCKS * CAP
TILE = 512
MESH = pl.DeviceIdType.MESH


def kernel(
    tokens_in, gain_in, router_in, experts_in, slots_in, w_in, w_out,
    update, gate,
    tokens, gain, router, experts, slots,
    send, recv, resp, back, win, wout, normed, acc, onehot,
    ready, small_sem, load_sem, pair_send, pair_recv, out_send, out_recv, back_send, back_recv,
):
    core = lax.axis_index("dp")
    me = lax.axis_index("expert")
    z, x, y = me // PLANE, lax.rem(me // YS, XS), lax.rem(me, YS)
    half = w_in.shape[2] // TILE

    def at(expert):
        return {"dp": core, "expert": expert}

    def blocks(chunk, sign, act, far_first=False, column=True, only=tuple(range(ZS))):
        for i, dz in enumerate(CHUNKS[chunk]):
            if dz not in only:
                continue
            plane = lax.rem(z + sign * dz + ZS, ZS) * PLANE
            base = (2 * chunk + i) * PLANE
            whole_column = column and dz != 0
            if not column and dz != 0:
                pl.semaphore_wait(ready.at[dz], 1)
            if not whole_column:
                for dy in range(1, YS):
                    act(base + dy, plane + x * YS + ys[sign][dy])

            def step(s, carry):
                t = XS - 1 - s
                dx = t + t // 2 - 2 * (t // 3) if far_first else s
                line = plane + lax.rem(x + sign * dx + XS, XS) * YS
                for dy in (2, 1, 3, 0) if far_first else range(YS):
                    act(base + dx * YS + dy, line + ys[sign][dy])
                return carry

            first = 0 if whole_column else 1
            lax.fori_loop(0 if far_first else first, XS - first if far_first else XS, step, 0)

    columns = tuple((ORDER.index(dz) * PLANE, dz, lax.rem(z + dz, ZS) * PLANE + x * YS + y) for dz in ORDER if dz)
    ys = {sign: [lax.rem(y + sign * dy + YS, YS) for dy in range(YS)] for sign in (1, -1)}

    def greet(k, expert):
        pl.semaphore_signal(barrier, inc=1, device_id=at(expert), device_id_type=MESH)

    small = []
    pieces = ((tokens_in, tokens), (gain_in, gain), (experts_in, experts), (slots_in, slots), (router_in, router))
    for i, (source, target) in enumerate(pieces):
        small.append(pltpu.make_async_copy(source, target, small_sem.at[i]))
        small[-1].start()

    barrier = pltpu.get_barrier_semaphore()
    partner = {"dp": 1 - core, "expert": me}
    pl.semaphore_signal(barrier, inc=1, device_id=partner, device_id_type=MESH)
    for k, dz, peer in columns:
        greet(k, peer)
    blocks(SELF_CHUNK, 1, greet, True, False, (0,))

    loads = []
    for t in range(half):
        cols = pl.ds(t * TILE, TILE)
        loads.append(pltpu.make_async_copy(w_in.at[0, :, cols], win.at[t], load_sem.at[0, t]))
        loads.append(pltpu.make_async_copy(w_out.at[0, cols, :], wout.at[t], load_sem.at[1, t]))
    for copy in loads:
        copy.start()

    for copy in small:
        copy.wait()
    values = tokens[...].astype(jnp.float32)
    mean = jnp.mean(values, axis=1, keepdims=True)
    centred = values - mean
    var = jnp.mean(centred * centred, axis=1, keepdims=True)
    normed[...] = (centred * lax.rsqrt(var + 1e-06) * gain[...]).astype(jnp.bfloat16)

    expert = experts[...]
    slot = slots[...]
    dz = (expert // PLANE - z) & (ZS - 1)
    dx = ((expert // YS) % XS - x) & (XS - 1)
    dy = (expert % YS - y) & (YS - 1)
    place = jnp.zeros_like(dz)
    for i, d in enumerate(ORDER):
        place = jnp.where(dz == d, i, place)
    rel = ((place * PLANE) + dx * YS + dy) * CAP + slot
    rel = jnp.where(slot >= 0, rel, -1)
    count = rel.shape[1]
    for chunk in range(len(CHUNKS)):
        rows = lax.broadcasted_iota(jnp.int32, (CHUNK_ROWS, count), 0) + chunk * CHUNK_ROWS
        pick = jnp.where(rows == rel, 1.0, 0.0).astype(jnp.bfloat16)
        picked = jnp.dot(pick, normed[...], preferred_element_type=jnp.float32)
        first = chunk * CHUNK_BLOCKS
        send[first : first + CHUNK_BLOCKS] = picked.reshape(CHUNK_BLOCKS, CAP, -1).astype(jnp.bfloat16)

    pl.semaphore_wait(barrier, len(columns) + PLANE)
    for k, dz, peer in columns:
        pl.semaphore_signal(ready.at[ZS - dz], inc=1, device_id=at(peer), device_id_type=MESH)

    def pair_copy(w, t, which):
        dst = (win, wout)[which].at[half + t]
        src = w.at[0, :, pl.ds(t * TILE, TILE)] if which == 0 else w.at[0, pl.ds(t * TILE, TILE), :]
        return pltpu.make_async_remote_copy(
            src_ref=src, dst_ref=dst, send_sem=pair_send.at[which, t], recv_sem=pair_recv.at[which, t],
            device_id=partner, device_id_type=MESH,
        )

    def dispatch(chunk):
        def act(k, expert):
            pltpu.make_async_remote_copy(
                src_ref=send.at[k], dst_ref=recv.at[k], send_sem=out_send, recv_sem=out_recv.at[chunk],
                device_id=at(expert), device_id_type=MESH,
            ).start()

        return act

    for k, dz, peer in columns:
        dispatch(ORDER.index(dz) // 2)(k, peer)
    pairs = []
    for chunk in range(len(CHUNKS)):
        blocks(chunk, 1, dispatch(chunk), column=False)
        if chunk == 0:
            pairs = [pair_copy((w_in, w_out)[s], t, s) for t in range(half) for s in (0, 1)]
            for copy in pairs:
                copy.start()
    recv[SELF] = send[SELF]

    eye = lax.broadcasted_iota(jnp.int32, (count, count), 0) == lax.broadcasted_iota(jnp.int32, (count, count), 1)

    def column(row):
        return jnp.sum(jnp.where(eye, row.astype(jnp.float32), 0.0), axis=1, keepdims=True).astype(jnp.int32)

    expert_col, rel_col = column(expert), column(rel)
    logits = jnp.dot(normed[...], router[...], preferred_element_type=jnp.float32)
    powers = jnp.exp(logits - jnp.max(logits, axis=1, keepdims=True))
    lanes = lax.broadcasted_iota(jnp.int32, powers.shape, 1)
    chosen = jnp.sum(jnp.where(lanes == expert_col, powers, 0.0), axis=1, keepdims=True)
    gate[...] = jnp.broadcast_to(chosen / jnp.sum(powers, axis=1, keepdims=True), gate.shape)
    for chunk in range(len(CHUNKS)):
        cols = lax.broadcasted_iota(jnp.int32, (count, CHUNK_ROWS), 1) + chunk * CHUNK_ROWS
        onehot[chunk] = jnp.where(cols == rel_col, 1.0, 0.0).astype(jnp.bfloat16)

    for copy in loads:
        copy.wait()

    def whole(src, dst, chunk, send_sem, recv_sem):
        first = chunk * CHUNK_BLOCKS
        many = CHUNK_BLOCKS - (1 if 0 in CHUNKS[chunk] else 0)
        return pltpu.make_async_remote_copy(
            src_ref=src.at[pl.ds(first, many)], dst_ref=dst.at[pl.ds(first, many)],
            send_sem=send_sem, recv_sem=recv_sem, device_id=partner, device_id_type=MESH,
        )

    for chunk in range(len(CHUNKS)):
        whole(send, recv, chunk, out_send, out_recv.at[chunk]).wait_recv()
        first = chunk * CHUNK_BLOCKS
        here = recv[first : first + CHUNK_BLOCKS].reshape(CHUNK_ROWS, -1)
        acc[...] = jnp.zeros_like(acc)

        def tile(t, carry):
            hidden = jnp.dot(here, win[t], preferred_element_type=jnp.float32)
            inner = 0.7978845608028654 * (hidden + 0.044715 * (hidden * hidden * hidden))
            hidden = (hidden * (0.5 * (1.0 + jnp.tanh(inner)))).astype(jnp.bfloat16)
            acc[...] += jnp.dot(hidden, wout[t], preferred_element_type=jnp.float32)
            return carry

        if chunk == 0:
            lax.fori_loop(0, half, tile, 0, unroll=2)
            for t in range(half):
                for copy in pairs[2 * t : 2 * t + 2]:
                    copy.wait_recv()
                tile(half + t, 0)
        else:
            lax.fori_loop(0, 2 * half, tile, 0, unroll=2)
        resp[first : first + CHUNK_BLOCKS] = acc[...].reshape(CHUNK_BLOCKS, CAP, -1).astype(jnp.bfloat16)

        def answer(k, expert):
            pltpu.make_async_remote_copy(
                src_ref=resp.at[k], dst_ref=back.at[k], send_sem=back_send, recv_sem=back_recv.at[chunk],
                device_id=at(expert), device_id_type=MESH,
            ).start()

        blocks(chunk, -1, answer, True)
    back[SELF] = resp[SELF]

    total = jnp.zeros(values.shape, jnp.float32)
    for chunk in range(len(CHUNKS)):
        whole(resp, back, chunk, back_send, back_recv.at[chunk]).wait_recv()
        first = chunk * CHUNK_BLOCKS
        rows = back[first : first + CHUNK_BLOCKS].reshape(CHUNK_ROWS, -1)
        total = total + jnp.dot(onehot[chunk], rows, preferred_element_type=jnp.float32)
    update[...] = total.astype(jnp.bfloat16)

    for copy in pairs:
        copy.wait_send()
    for chunk in range(len(CHUNKS)):
        whole(send, recv, chunk, out_send, out_recv.at[chunk]).wait_send()
        whole(resp, back, chunk, back_send, back_recv.at[chunk]).wait_send()


def finish(tokens, gate, total, mixed, update):
    update[...] = total[...]
    values = tokens[...].astype(jnp.float32)
    mixed[...] = (values + gate[:, :1] * total[...].astype(jnp.float32)).astype(jnp.bfloat16)


def per_device(tokens, ln_gain, router_weight, routes_expert, route_slot, w_in, w_out):
    count, width = tokens.shape
    half = w_in.shape[2] // TILE
    vmem = pl.BlockSpec(memory_space=pltpu.VMEM)
    hbm = pl.BlockSpec(memory_space=pltpu.MemorySpace.HBM)
    blocks = (EXPERTS, CAP, width)
    dma = pltpu.SemaphoreType.DMA
    shape = jax.ShapeDtypeStruct(tokens.shape, jnp.bfloat16)
    total, gate = pl.pallas_call(
        kernel,
        out_shape=(pltpu.VMEM(tokens.shape, jnp.bfloat16), pltpu.VMEM((count, 128), jnp.float32)),
        in_specs=[hbm] * 7,
        out_specs=(vmem, vmem),
        scratch_shapes=[
            pltpu.VMEM(tokens.shape, jnp.bfloat16),
            pltpu.VMEM((1, width), jnp.float32),
            pltpu.VMEM(router_weight.shape, jnp.bfloat16),
            pltpu.VMEM((1, count), jnp.int32),
            pltpu.VMEM((1, count), jnp.int32),
            pltpu.VMEM(blocks, jnp.bfloat16),
            pltpu.VMEM(blocks, jnp.bfloat16),
            pltpu.VMEM(blocks, jnp.bfloat16),
            pltpu.VMEM(blocks, jnp.bfloat16),
            pltpu.VMEM((2 * half, width, TILE), jnp.bfloat16),
            pltpu.VMEM((2 * half, TILE, width), jnp.bfloat16),
            pltpu.VMEM((count, width), jnp.bfloat16),
            pltpu.VMEM((CHUNK_ROWS, width), jnp.float32),
            pltpu.VMEM((len(CHUNKS), count, CHUNK_ROWS), jnp.bfloat16),
            pltpu.SemaphoreType.REGULAR((ZS,)), dma((5,)), dma((2, half)), dma((2, half)), dma((2, half)),
            dma, dma((len(CHUNKS),)), dma, dma((len(CHUNKS),)),
        ],
        compiler_params=pltpu.CompilerParams(
            collective_id=0, has_side_effects=True, vmem_limit_bytes=32 * 1024 * 1024
        ),
    )(
        *(
            pltpu.with_memory_space_constraint(value, pltpu.MemorySpace.HBM)
            for value in (
                tokens, ln_gain.reshape(1, -1), router_weight,
                routes_expert.reshape(1, -1), route_slot.reshape(1, -1), w_in, w_out,
            )
        )
    )
    return pl.pallas_call(
        finish,
        out_shape=(shape, shape),
        grid=(2,),
        in_specs=[pl.BlockSpec((count // 2, n), lambda i: (i, 0)) for n in (width, 128, width)],
        out_specs=(pl.BlockSpec((count // 2, width), lambda i: (i, 0)),) * 2,
        compiler_params=pltpu.CompilerParams(vmem_limit_bytes=8 * 1024 * 1024),
    )(tokens, gate, total)


def solution(mesh):
    in_specs = (
        P(("dp", "expert"), None),
        P(),
        P(),
        P(("dp", "expert")),
        P(("dp", "expert")),
        P("expert", None, "dp"),
        P("expert", "dp", None),
    )
    out_specs = (P(("dp", "expert"), None), P(("dp", "expert"), None))
    return jax.shard_map(
        per_device, mesh=mesh, in_specs=in_specs, out_specs=out_specs, check_vma=False
    )
```

```python
import functools

import jax
import jax.numpy as jnp
from jax import lax
from jax.experimental import pallas as pl
from jax.experimental.pallas import tpu as pltpu
from jax.sharding import PartitionSpec as P

CAP = 4
ZS, XS, YS = 8, 4, 4
PLANE = XS * YS
EXPERTS = ZS * PLANE
SLOTS = EXPERTS * CAP
CHUNKS = ((2, 6), (3, 5), (0, 4), (1, 7))
ORDER = tuple(dz for pair in CHUNKS for dz in pair)
SELF = ORDER.index(0) * PLANE
SELF_CHUNK = ORDER.index(0) // 2
CHUNK_BLOCKS = 2 * PLANE
CHUNK_ROWS = CHUNK_BLOCKS * CAP
TILE = 512
MESH = pl.DeviceIdType.MESH


def kernel(
    tokens_in, gain_in, router_in, experts_in, slots_in, w_in, w_out,
    update, gate,
    tokens, gain, router, experts, slots,
    send, recv, resp, back, win, wout, normed, acc, onehot,
    ready, small_sem, load_sem, pair_send, pair_recv, out_send, out_recv, back_send, back_recv,
):
    core = lax.axis_index("dp")
    me = lax.axis_index("expert")
    z, x, y = me // PLANE, lax.rem(me // YS, XS), lax.rem(me, YS)
    half = w_in.shape[2] // TILE

    def at(expert):
        return {"dp": core, "expert": expert}

    def blocks(chunk, sign, act, far_first=False, column=True, only=tuple(range(ZS))):
        for i, dz in enumerate(CHUNKS[chunk]):
            if dz not in only:
                continue
            plane = lax.rem(z + sign * dz + ZS, ZS) * PLANE
            base = (2 * chunk + i) * PLANE
            whole_column = column and dz != 0
            if not column and dz != 0:
                pl.semaphore_wait(ready.at[dz], 1)
            if not whole_column:
                for dy in range(1, YS):
                    act(base + dy, plane + x * YS + ys[sign][dy])

            def step(s, carry):
                t = XS - 1 - s
                dx = t + t // 2 - 2 * (t // 3) if far_first else s
                line = plane + lax.rem(x + sign * dx + XS, XS) * YS
                for dy in (2, 1, 3, 0) if far_first else range(YS):
                    act(base + dx * YS + dy, line + ys[sign][dy])
                return carry

            first = 0 if whole_column else 1
            lax.fori_loop(0 if far_first else first, XS - first if far_first else XS, step, 0)

    columns = tuple((ORDER.index(dz) * PLANE, dz, lax.rem(z + dz, ZS) * PLANE + x * YS + y) for dz in ORDER if dz)
    ys = {sign: [lax.rem(y + sign * dy + YS, YS) for dy in range(YS)] for sign in (1, -1)}

    def greet(k, expert):
        pl.semaphore_signal(barrier, inc=1, device_id=at(expert), device_id_type=MESH)

    small = []
    pieces = ((tokens_in, tokens), (gain_in, gain), (experts_in, experts), (slots_in, slots), (router_in, router))
    for i, (source, target) in enumerate(pieces):
        small.append(pltpu.make_async_copy(source, target, small_sem.at[i]))
        small[-1].start()

    barrier = pltpu.get_barrier_semaphore()
    partner = {"dp": 1 - core, "expert": me}
    pl.semaphore_signal(barrier, inc=1, device_id=partner, device_id_type=MESH)
    for k, dz, peer in columns:
        greet(k, peer)
    blocks(SELF_CHUNK, 1, greet, True, False, (0,))

    for copy in small:
        copy.wait()
    values = tokens[...].astype(jnp.float32)
    mean = jnp.mean(values, axis=1, keepdims=True)
    centred = values - mean
    var = jnp.mean(centred * centred, axis=1, keepdims=True)
    normed[...] = (centred * lax.rsqrt(var + 1e-06) * gain[...]).astype(jnp.bfloat16)

    expert = experts[...]
    slot = slots[...]
    dz = (expert // PLANE - z) & (ZS - 1)
    dx = ((expert // YS) % XS - x) & (XS - 1)
    dy = (expert % YS - y) & (YS - 1)
    place = jnp.zeros_like(dz)
    for i, d in enumerate(ORDER):
        place = jnp.where(dz == d, i, place)
    rel = ((place * PLANE) + dx * YS + dy) * CAP + slot
    rel = jnp.where(slot >= 0, rel, -1)
    count = rel.shape[1]
    for chunk in range(len(CHUNKS)):
        rows = lax.broadcasted_iota(jnp.int32, (CHUNK_ROWS, count), 0) + chunk * CHUNK_ROWS
        pick = jnp.where(rows == rel, 1.0, 0.0).astype(jnp.bfloat16)
        picked = jnp.dot(pick, normed[...], preferred_element_type=jnp.float32)
        first = chunk * CHUNK_BLOCKS
        send[first : first + CHUNK_BLOCKS] = picked.reshape(CHUNK_BLOCKS, CAP, -1).astype(jnp.bfloat16)

    pl.semaphore_wait(barrier, len(columns) + PLANE)
    for k, dz, peer in columns:
        pl.semaphore_signal(ready.at[ZS - dz], inc=1, device_id=at(peer), device_id_type=MESH)

    def pair_copy(w, t, which):
        dst = (win, wout)[which].at[half + t]
        src = w.at[0, :, pl.ds(t * TILE, TILE)] if which == 0 else w.at[0, pl.ds(t * TILE, TILE), :]
        return pltpu.make_async_remote_copy(
            src_ref=src, dst_ref=dst, send_sem=pair_send.at[which, t], recv_sem=pair_recv.at[which, t],
            device_id=partner, device_id_type=MESH,
        )

    def dispatch(chunk):
        def act(k, expert):
            pltpu.make_async_remote_copy(
                src_ref=send.at[k], dst_ref=recv.at[k], send_sem=out_send, recv_sem=out_recv.at[chunk],
                device_id=at(expert), device_id_type=MESH,
            ).start()

        return act

    for k, dz, peer in columns:
        dispatch(ORDER.index(dz) // 2)(k, peer)
    pairs = []
    for chunk in range(len(CHUNKS)):
        blocks(chunk, 1, dispatch(chunk), column=False)
        if chunk == 0:
            pairs = [pair_copy((w_in, w_out)[s], t, s) for t in range(half) for s in (0, 1)]
            for copy in pairs:
                copy.start()
    recv[SELF] = send[SELF]

    loads = []
    for t in range(half):
        cols = pl.ds(t * TILE, TILE)
        loads.append(pltpu.make_async_copy(w_in.at[0, :, cols], win.at[t], load_sem.at[0, t]))
        loads.append(pltpu.make_async_copy(w_out.at[0, cols, :], wout.at[t], load_sem.at[1, t]))
    for copy in loads:
        copy.start()

    eye = lax.broadcasted_iota(jnp.int32, (count, count), 0) == lax.broadcasted_iota(jnp.int32, (count, count), 1)

    def column(row):
        return jnp.sum(jnp.where(eye, row.astype(jnp.float32), 0.0), axis=1, keepdims=True).astype(jnp.int32)

    expert_col, rel_col = column(expert), column(rel)
    logits = jnp.dot(normed[...], router[...], preferred_element_type=jnp.float32)
    powers = jnp.exp(logits - jnp.max(logits, axis=1, keepdims=True))
    lanes = lax.broadcasted_iota(jnp.int32, powers.shape, 1)
    chosen = jnp.sum(jnp.where(lanes == expert_col, powers, 0.0), axis=1, keepdims=True)
    gate[...] = jnp.broadcast_to(chosen / jnp.sum(powers, axis=1, keepdims=True), gate.shape)
    for chunk in range(len(CHUNKS)):
        cols = lax.broadcasted_iota(jnp.int32, (count, CHUNK_ROWS), 1) + chunk * CHUNK_ROWS
        onehot[chunk] = jnp.where(cols == rel_col, 1.0, 0.0).astype(jnp.bfloat16)

    for copy in loads:
        copy.wait()

    def whole(src, dst, chunk, send_sem, recv_sem):
        first = chunk * CHUNK_BLOCKS
        many = CHUNK_BLOCKS - (1 if 0 in CHUNKS[chunk] else 0)
        return pltpu.make_async_remote_copy(
            src_ref=src.at[pl.ds(first, many)], dst_ref=dst.at[pl.ds(first, many)],
            send_sem=send_sem, recv_sem=recv_sem, device_id=partner, device_id_type=MESH,
        )

    for chunk in range(len(CHUNKS)):
        whole(send, recv, chunk, out_send, out_recv.at[chunk]).wait_recv()
        first = chunk * CHUNK_BLOCKS
        here = recv[first : first + CHUNK_BLOCKS].reshape(CHUNK_ROWS, -1)
        acc[...] = jnp.zeros_like(acc)

        def tile(t, carry):
            hidden = jnp.dot(here, win[t], preferred_element_type=jnp.float32)
            inner = 0.7978845608028654 * (hidden + 0.044715 * (hidden * hidden * hidden))
            hidden = (hidden * (0.5 * (1.0 + jnp.tanh(inner)))).astype(jnp.bfloat16)
            acc[...] += jnp.dot(hidden, wout[t], preferred_element_type=jnp.float32)
            return carry

        if chunk == 0:
            lax.fori_loop(0, half, tile, 0, unroll=2)
            for t in range(half):
                for copy in pairs[2 * t : 2 * t + 2]:
                    copy.wait_recv()
                tile(half + t, 0)
        else:
            lax.fori_loop(0, 2 * half, tile, 0, unroll=2)
        resp[first : first + CHUNK_BLOCKS] = acc[...].reshape(CHUNK_BLOCKS, CAP, -1).astype(jnp.bfloat16)

        def answer(k, expert):
            pltpu.make_async_remote_copy(
                src_ref=resp.at[k], dst_ref=back.at[k], send_sem=back_send, recv_sem=back_recv.at[chunk],
                device_id=at(expert), device_id_type=MESH,
            ).start()

        blocks(chunk, -1, answer, True)
    back[SELF] = resp[SELF]

    total = jnp.zeros(values.shape, jnp.float32)
    for chunk in range(len(CHUNKS)):
        whole(resp, back, chunk, back_send, back_recv.at[chunk]).wait_recv()
        first = chunk * CHUNK_BLOCKS
        rows = back[first : first + CHUNK_BLOCKS].reshape(CHUNK_ROWS, -1)
        total = total + jnp.dot(onehot[chunk], rows, preferred_element_type=jnp.float32)
    update[...] = total.astype(jnp.bfloat16)

    for copy in pairs:
        copy.wait_send()
    for chunk in range(len(CHUNKS)):
        whole(send, recv, chunk, out_send, out_recv.at[chunk]).wait_send()
        whole(resp, back, chunk, back_send, back_recv.at[chunk]).wait_send()


def finish(tokens, gate, total, mixed, update):
    update[...] = total[...]
    values = tokens[...].astype(jnp.float32)
    mixed[...] = (values + gate[:, :1] * total[...].astype(jnp.float32)).astype(jnp.bfloat16)


def per_device(tokens, ln_gain, router_weight, routes_expert, route_slot, w_in, w_out):
    count, width = tokens.shape
    half = w_in.shape[2] // TILE
    vmem = pl.BlockSpec(memory_space=pltpu.VMEM)
    hbm = pl.BlockSpec(memory_space=pltpu.MemorySpace.HBM)
    blocks = (EXPERTS, CAP, width)
    dma = pltpu.SemaphoreType.DMA
    shape = jax.ShapeDtypeStruct(tokens.shape, jnp.bfloat16)
    total, gate = pl.pallas_call(
        kernel,
        out_shape=(pltpu.VMEM(tokens.shape, jnp.bfloat16), pltpu.VMEM((count, 128), jnp.float32)),
        in_specs=[hbm] * 7,
        out_specs=(vmem, vmem),
        scratch_shapes=[
            pltpu.VMEM(tokens.shape, jnp.bfloat16),
            pltpu.VMEM((1, width), jnp.float32),
            pltpu.VMEM(router_weight.shape, jnp.bfloat16),
            pltpu.VMEM((1, count), jnp.int32),
            pltpu.VMEM((1, count), jnp.int32),
            pltpu.VMEM(blocks, jnp.bfloat16),
            pltpu.VMEM(blocks, jnp.bfloat16),
            pltpu.VMEM(blocks, jnp.bfloat16),
            pltpu.VMEM(blocks, jnp.bfloat16),
            pltpu.VMEM((2 * half, width, TILE), jnp.bfloat16),
            pltpu.VMEM((2 * half, TILE, width), jnp.bfloat16),
            pltpu.VMEM((count, width), jnp.bfloat16),
            pltpu.VMEM((CHUNK_ROWS, width), jnp.float32),
            pltpu.VMEM((len(CHUNKS), count, CHUNK_ROWS), jnp.bfloat16),
            pltpu.SemaphoreType.REGULAR((ZS,)), dma((5,)), dma((2, half)), dma((2, half)), dma((2, half)),
            dma, dma((len(CHUNKS),)), dma, dma((len(CHUNKS),)),
        ],
        compiler_params=pltpu.CompilerParams(
            collective_id=0, has_side_effects=True, vmem_limit_bytes=32 * 1024 * 1024
        ),
    )(
        *(
            pltpu.with_memory_space_constraint(value, pltpu.MemorySpace.HBM)
            for value in (
                tokens, ln_gain.reshape(1, -1), router_weight,
                routes_expert.reshape(1, -1), route_slot.reshape(1, -1), w_in, w_out,
            )
        )
    )
    return pl.pallas_call(
        finish,
        out_shape=(shape, shape),
        grid=(2,),
        in_specs=[pl.BlockSpec((count // 2, n), lambda i: (i, 0)) for n in (width, 128, width)],
        out_specs=(pl.BlockSpec((count // 2, width), lambda i: (i, 0)),) * 2,
        compiler_params=pltpu.CompilerParams(vmem_limit_bytes=8 * 1024 * 1024),
    )(tokens, gate, total)


def solution(mesh):
    in_specs = (
        P(("dp", "expert"), None),
        P(),
        P(),
        P(("dp", "expert")),
        P(("dp", "expert")),
        P("expert", None, "dp"),
        P("expert", "dp", None),
    )
    out_specs = (P(("dp", "expert"), None), P(("dp", "expert"), None))
    return jax.shard_map(
        per_device, mesh=mesh, in_specs=in_specs, out_specs=out_specs, check_vma=False
    )
```
